256 devices in a mesh: col: 16 (over x, y_lo, core), row: 16 (over z, y_hi).
Axes of the slice: x: 4, y: 4 (y_hi: 2, y_lo: 2; y = y_hi * 2 + y_lo), z: 8, core: 2. Of those that a mesh axis runs over, the one named last changes fastest.
Arguments:
- visibilities: bfloat16 [2, 16384, 16384], P(None, 'col', 'row'), may hold values from -6 to 6
- col_offsets: int32 [16], P('col'), may hold values from 0 to 15360
- row_offsets: int32 [16], replicated, may hold values from 0 to 15360
- facet_offsets: int32 [16, 2], replicated, may hold values from 0 to 16383
- facet_order: int32 [16], replicated, may hold values from 0 to 15, each once
- vis_counts: int32 [16, 16], P('col', 'row'), may hold values from 512 to 1024
Outputs:
- facet_images: float32 [16, 2, 64, 4096], P('col', None, None, 'row')
- peak: float32 [16], P('col')
The draws below stay inside these ranges and needn't reach their ends.
Inputs may be any that keep to these rules, and one draw needn't show every extreme that they name: `facet_order`: each slot names a different facet.
All inputs are finite; a program needn't handle non-finite values.
Results may differ from the reference program's by a relative error of at most 0.0078.
Values may be sent and summed in bfloat16 or wider, within the bound.
A program may use at most 128 MiB of HBM per device.

```python
import math
import jax
import jax.numpy as jnp
from jax import lax

M = 1024
FS = 4096
NG = 16384
FR = 64
NFACET = 16
N_COL = 16
N_ROW = 16


def with_ends(entries, rng, least, largest):
    extent = entries.shape
    place = [jax.random.randint(jax.random.fold_in(rng, axis), (), 0, extent[axis]) for axis in range(len(extent))]
    entries = entries.at[tuple(place)].set(least)
    longest = extent.index(max(extent))
    place[longest] = (place[longest] + 1) % extent[longest]
    return entries.at[tuple(place)].set(largest)


def steps_of(key, dims, pieces, low, high):
    gain = 1.0
    for dim, blocks in pieces:
        steps = jax.random.uniform(jax.random.fold_in(jax.random.fold_in(key, 6), dim), (blocks,), jnp.float32, low / len(pieces), high / len(pieces))
        gain = gain * jnp.repeat(jnp.exp(steps), dims[dim] // blocks).reshape((-1,) + (1,) * (len(dims) - 1 - dim))
    return gain


def noise(own_key, shape, width, reach, cuts=(), kind=jnp.bfloat16):
    result = jax.random.normal(own_key, shape, jnp.float32) * width
    if len(cuts) > 0:
        result = steps_of(own_key, shape, cuts, -0.22, 0.18) * result
    return jnp.clip(result, min=-reach, max=reach).astype(kind)


def setup_inputs(seed: int = 0) -> dict:
    arg_keys = jax.random.split(jax.random.key(seed), 7)
    return {
        "visibilities": noise(arg_keys[0], (2, N_COL * M, N_ROW * M), 1.0, 6.0, ((1, 16), (2, 16))),
        "col_offsets": with_ends(jax.random.randint(arg_keys[1], (N_COL,), 0, NG - M + 1), jax.random.fold_in(arg_keys[1], 1), 0, NG - M).astype(jnp.int32),
        "row_offsets": with_ends(jax.random.randint(arg_keys[2], (N_ROW,), 0, NG - M + 1), jax.random.fold_in(arg_keys[2], 1), 0, NG - M).astype(jnp.int32),
        "facet_offsets": with_ends(jax.random.randint(arg_keys[3], (NFACET, 2), 0, NG), jax.random.fold_in(arg_keys[3], 1), 0, NG - 1).astype(jnp.int32),
        "facet_order": jax.random.permutation(arg_keys[4], NFACET).astype(jnp.int32),
        "vis_counts": with_ends(jax.random.randint(arg_keys[5], (N_COL, N_ROW), M // 2, M + 1), jax.random.fold_in(arg_keys[5], 1), M // 2, M).astype(jnp.int32),
    }


TWO_PI = 2.0 * math.pi
BEAM_SLOPE = 0.66

def phase_table(first_ids, second_ids, factor):
    product = first_ids[:, None] * second_ids[None, :] % NG
    angles = product.astype(jnp.float32) * (TWO_PI / NG)
    return ((jnp.cos(angles) * factor).astype(jnp.bfloat16), (jnp.sin(angles) * factor).astype(jnp.bfloat16))

def complex_product(left_real, left_imag, right_real, right_imag):
    left_rows = jnp.concatenate([left_real, left_imag], axis=0)
    right_cols = jnp.concatenate([right_real, right_imag], axis=1)
    product = jnp.dot(left_rows, right_cols, preferred_element_type=jnp.float32)
    product = product.reshape(2, left_real.shape[0], 2, right_real.shape[1])
    real_part = product[0, :, 0] - product[1, :, 1]
    imag_part = product[0, :, 1] + product[1, :, 0]
    return (real_part, imag_part)

def reference(visibilities, col_offsets, row_offsets, facet_offsets, facet_order, vis_counts):
    slot_pick = (facet_order[:, None] == jnp.arange(NFACET, dtype=jnp.int32)[None, :]).astype(jnp.int32)
    slot_offsets = lax.optimization_barrier(jnp.sum(slot_pick[:, :, None] * facet_offsets[None, :, :], axis=1))
    row_ids = jnp.arange(M, dtype=jnp.int32)
    pixel_rows = jnp.arange(FR, dtype=jnp.int32) + (FS // 2 - FR // 2)
    pixel_cols = jnp.arange(FS, dtype=jnp.int32)
    grid_u = (col_offsets[:, None] + row_ids[None, :]).reshape(N_COL * M)
    first_scale = 1.0 / math.sqrt(M * N_COL)
    second_scale = 0.5 / math.sqrt(M * N_ROW)

    def add_row(running, row_index):
        column_strip = lax.dynamic_slice_in_dim(visibilities, (row_index * M).astype(jnp.int32), M, 2)
        counts_here = lax.dynamic_index_in_dim(vis_counts, row_index, 1, keepdims=False)
        live_rows = (row_ids[None, :] < counts_here[:, None]).reshape(N_COL * M)
        column_strip = jnp.where(live_rows[None, :, None], column_strip, jnp.zeros_like(column_strip))
        grid_v = lax.dynamic_index_in_dim(row_offsets, row_index, 0, keepdims=False) + row_ids

        def one_slot(slot_index):
            offsets = lax.dynamic_index_in_dim(slot_offsets, slot_index, 0, keepdims=False)
            image_rows = (offsets[0] + pixel_rows) % NG
            table_real, table_imag = phase_table(image_rows, grid_u, first_scale)
            part_real, part_imag = complex_product(table_real, table_imag, column_strip[0], column_strip[1])
            columns = jnp.stack([part_real, part_imag], axis=0).astype(jnp.bfloat16)
            image_cols = (offsets[1] + pixel_cols) % NG
            second_real, second_imag = phase_table(grid_v, image_cols, second_scale)
            out_real, out_imag = complex_product(columns[0], columns[1], second_real, second_imag)
            return jnp.stack([out_real, out_imag], axis=0)
        return (running + lax.map(one_slot, jnp.arange(NFACET, dtype=jnp.int32)), None)
    initial = jnp.zeros((NFACET, 2, FR, FS), jnp.float32)
    facet_sum, ignored = lax.scan(add_row, initial, jnp.arange(N_ROW, dtype=jnp.int32))
    beam = 1.0 - BEAM_SLOPE * (pixel_cols.astype(jnp.float32) + 0.5) / FS
    facet_images = facet_sum / beam[None, None, None, :]
    magnitude = jnp.sqrt(facet_images[:, 0] * facet_images[:, 0] + facet_images[:, 1] * facet_images[:, 1])
    peak = lax.optimization_barrier(jnp.max(magnitude, axis=(1, 2)))
    return (facet_images, peak)
```

```python
import math

import jax
import jax.numpy as jnp
from jax import lax
from jax.sharding import PartitionSpec as P

M = 1024
FS = 4096
NG = 16384
FR = 64


TWO_PI = 2.0 * math.pi
BEAM_SLOPE = 0.66


def in_blocks(x, dim, length):
    before, after = (x.shape[:dim], x.shape[dim + 1 :])
    return jnp.moveaxis(x.reshape(*before, length, -1, *after), dim, 0)


def sent_and_summed(x, axis):
    arrived = lax.all_to_all(x, axis, split_axis=0, concat_axis=0, tiled=True)
    return arrived.astype(jnp.float32).sum(axis=0)


def wave(first_ids, second_ids, factor=1.0):
    product = first_ids[:, None] * second_ids[None, :] % NG
    angles = product.astype(jnp.float32) * (TWO_PI / NG)
    return jnp.cos(angles) * factor, jnp.sin(angles) * factor


def times(a, b):
    return a[0] * b[0] - a[1] * b[1], a[0] * b[1] + a[1] * b[0]


def local(visibilities, col_offsets, row_offsets, facet_offsets, facet_order, vis_counts):
    col_count = lax.axis_size("col")
    row_count = lax.axis_size("row")
    col_index = lax.axis_index("col")
    row_index = lax.axis_index("row")
    facets = facet_order.shape[0]
    block_cols = FS // row_count
    slot_pick = (facet_order[:, None] == jnp.arange(facets, dtype=jnp.int32)[None, :]).astype(jnp.int32)
    slot_offsets = jnp.sum(slot_pick[:, :, None] * facet_offsets[None, :, :], axis=1)
    own_pick = (jnp.arange(facets, dtype=jnp.int32) == col_index).astype(jnp.int32)
    own_facet = jnp.sum(slot_offsets * own_pick[:, None], axis=0)
    row_pick = (jnp.arange(row_count, dtype=jnp.int32) == row_index).astype(jnp.int32)
    row_shift = jnp.sum(row_offsets * row_pick)
    ids = jnp.arange(M, dtype=jnp.int32)
    live = (ids < vis_counts[0, 0]).astype(jnp.float32)
    first_scale = 1.0 / math.sqrt(M * col_count)
    second_scale = 0.5 / math.sqrt(M * row_count)

    grid_u = col_offsets[0] + ids
    base = wave((slot_offsets[:, 0] + (FS // 2 - FR // 2)) % NG, grid_u, first_scale)
    base = (base[0] * live, base[1] * live)
    steps = wave(jnp.arange(FR, dtype=jnp.int32), grid_u)
    re, im = times((base[0][:, None, :], base[1][:, None, :]), (steps[0][None], steps[1][None]))
    re, im = re.astype(jnp.bfloat16), im.astype(jnp.bfloat16)
    table = jnp.stack([jnp.concatenate([re, -im], axis=-1), jnp.concatenate([im, re], axis=-1)], axis=1)
    part = jnp.dot(
        table.reshape(facets * 2 * FR, 2 * M),
        visibilities.reshape(2 * M, M),
        preferred_element_type=jnp.float32,
    ).astype(jnp.bfloat16)
    columns = sent_and_summed(part.reshape(facets, 2, FR, M), "col")

    grid_v = row_shift + ids
    blocks = jnp.arange(row_count, dtype=jnp.int32)
    twist = wave((own_facet[1] + blocks * block_cols) % NG, grid_v, second_scale)
    fine = wave(grid_v, jnp.arange(block_cols, dtype=jnp.int32))
    fine_re, fine_im = fine[0].astype(jnp.bfloat16), fine[1].astype(jnp.bfloat16)
    right = jnp.concatenate(
        [jnp.concatenate([fine_re, fine_im], axis=1), jnp.concatenate([-fine_im, fine_re], axis=1)], axis=0
    )
    re, im = times((columns[0][None], columns[1][None]), (twist[0][:, None, :], twist[1][:, None, :]))
    left = jnp.concatenate([re, im], axis=-1).astype(jnp.bfloat16).reshape(row_count * FR, 2 * M)
    out = jnp.dot(left, right, preferred_element_type=jnp.float32).astype(jnp.bfloat16)
    facet_block = sent_and_summed(out.reshape(row_count, FR, 2 * block_cols), "row")
    facet_block = jnp.stack([facet_block[:, :block_cols], facet_block[:, block_cols:]])
    beam_cols = (row_index * block_cols + jnp.arange(block_cols, dtype=jnp.int32)).astype(jnp.float32)
    beam = 1.0 - BEAM_SLOPE * (beam_cols + 0.5) / FS
    facet_images = facet_block / beam[None, None, :]
    magnitude = jnp.sqrt(facet_images[0] * facet_images[0] + facet_images[1] * facet_images[1])
    peak = lax.pmax(jnp.max(magnitude)[None], "row")
    return (facet_images[None], peak)


def solution(mesh):
    in_specs = (P(None, "col", "row"), P("col"), P(), P(), P(), P("col", "row"))
    out_specs = (P("col", None, None, "row"), P("col"))
    return jax.shard_map(local, mesh=mesh, in_specs=in_specs, out_specs=out_specs, check_vma=False)
```

```python
import math

import jax
import jax.numpy as jnp
from jax import lax
from jax.experimental import pallas as pl
from jax.experimental.pallas import tpu as pltpu
from jax.sharding import PartitionSpec as P

MESH = pl.DeviceIdType.MESH
F32, BF16, I32 = jnp.float32, jnp.bfloat16, jnp.int32

M = 1024
FS = 4096
NG = 16384
FR = 64
NF = 16
CH = 16
NCH = FR // CH
JB = FS // NF
TWO_PI = 2.0 * math.pi
BEAM_SLOPE = 0.66
FIRST_SCALE = 1.0 / math.sqrt(NG)
SECOND_SCALE = 0.5 / math.sqrt(NG)

CORE, XA_UP, XB_UP, XA_DN, XB_DN, XC_UP, XC_DN, YLO, YHI, ZUP, ZDN = 0, 1, 2, 3, 4, 5, 6, 7, 8, 9, 13
COPIES = 17


def wave(exponent):
    angle = (exponent & (NG - 1)).astype(F32) * (TWO_PI / NG)
    return jnp.cos(angle), jnp.sin(angle)


def times(a, b):
    return a[0] * b[0] - a[1] * b[1], a[0] * b[1] + a[1] * b[0]


def iota(shape, dim):
    return lax.broadcasted_iota(I32, shape, dim)


def column_of(scalars, shape):
    row = iota(shape, 0)
    picked = jnp.zeros(shape, I32)
    for index, value in enumerate(scalars):
        picked = jnp.where(row == index, value, picked)
    return picked


def body(
    vis, col_offsets, row_offsets, facet_offsets, facet_order, vis_counts,
    out, peak,
    grid, table, unit_re, unit_im, part, part_in, own,
    xa_send, xb_send, xc_send, xa_recv, xb_recv, xc_recv, y_send, y_recv,
    twist_re, twist_im, left, fine, image, z_send, z_recv, h_send, h_recv, top, tops,
    load_sem, send_sem, recv_sem, top_send, top_recv,
):
    c, r = lax.axis_index("col"), lax.axis_index("row")
    x, ylo, core = c // 4, (c // 2) % 2, c % 2
    z, yhi = r // 2, r % 2
    to_core = (c + 1 - 2 * core, r)
    to_ylo = (c + 2 - 4 * ylo, r)
    to_yhi = (c, r + 1 - 2 * yhi)
    x_up, x_dn = ((c + 4) % 16, r), ((c + 12) % 16, r)
    z_up, z_dn = (c, (r + 2) % 16), (c, (r + 14) % 16)

    loads = [pltpu.make_async_copy(vis.at[p], grid.at[p], load_sem.at[p]) for p in range(2)]
    for load in loads:
        load.start()
    barrier = pltpu.get_barrier_semaphore()
    for peer in (to_core, to_ylo, x_up, x_dn):
        pl.semaphore_signal(barrier, inc=1, device_id=peer, device_id_type=MESH)
    for step in range(1, NF):
        pl.semaphore_signal(barrier, inc=1, device_id=(c, (r + step) % NF), device_id_type=MESH)

    started = []

    def send(src, dst, k, index, peer):
        copy = pltpu.make_async_remote_copy(
            src_ref=src, dst_ref=dst, send_sem=send_sem.at[k, index], recv_sem=recv_sem.at[k, index],
            device_id=peer, device_id_type=MESH,
        )
        copy.start()
        started.append(copy)
        return copy

    slots = [
        ((x + dx) % 4) * 4 + ((ylo + dy) % 2) * 2 + (core + 1 - half) % 2
        for half in range(2) for dx in range(4) for dy in range(2)
    ]
    rows_at = [facet_offsets[facet_order[s], 0] + (FS // 2 - FR // 2) for s in slots]
    wide = (NF, M)
    place = iota(wide, 1)
    grid_u = col_offsets[0] + place
    live = (place < vis_counts[0, 0]).astype(F32) * FIRST_SCALE
    slot_rows = column_of(rows_at, wide)
    unit = wave(grid_u * iota(wide, 0))
    unit_re[...], unit_im[...] = unit

    copies = [dict() for _ in range(NCH)]

    def build(k):
        base = wave(grid_u * ((slot_rows + CH * k) & (NG - 1)))
        base = (base[0] * live, base[1] * live)
        for half in range(2):
            for dx in range(4):
                for dy in range(2):
                    s = half * 8 + dx * 2 + dy
                    re, im = times((base[0][s : s + 1], base[1][s : s + 1]), (unit_re[...], unit_im[...]))
                    re, im = re.astype(BF16), im.astype(BF16)
                    table[half, dx, 0, dy, :, :M] = re
                    table[half, dx, 0, dy, :, M:] = -im
                    table[half, dx, 1, dy, :, :M] = im
                    table[half, dx, 1, dy, :, M:] = re

    def multiply(half):
        return jnp.dot(
            table[half].reshape(16 * CH, 2 * M), grid[...].reshape(2 * M, M), preferred_element_type=F32
        ).reshape(4, 2, 2, CH, M)

    def first(k):
        build(k)
        part[k] = multiply(0).astype(BF16)
        if k == 0:
            pl.semaphore_wait(barrier, 4 + NF - 1)
        copies[k]["core"] = send(part.at[k], part_in.at[k], k, CORE, to_core)
        own[k] = multiply(1)

    def spread_x(k):
        copies[k]["core"].wait_recv()
        xa_send[k, 0] = (own[k, 2, 0] + part_in[k, 2, 0].astype(F32)).astype(BF16)
        copies[k]["xa_up"] = send(xa_send.at[k, 0], xa_recv.at[k, 0], k, XA_UP, x_up)
        xa_send[k, 1] = (own[k, 2, 1] + part_in[k, 2, 1].astype(F32)).astype(BF16)
        copies[k]["xa_dn"] = send(xa_send.at[k, 1], xa_recv.at[k, 1], k, XA_DN, x_dn)
        xb_send[k, 0] = (own[k, 1, 1] + part_in[k, 1, 1].astype(F32)).astype(BF16)
        copies[k]["xb_up"] = send(xb_send.at[k, 0], xb_recv.at[k, 0], k, XB_UP, x_up)
        xb_send[k, 1] = (own[k, 3, 0] + part_in[k, 3, 0].astype(F32)).astype(BF16)
        copies[k]["xb_dn"] = send(xb_send.at[k, 1], xb_recv.at[k, 1], k, XB_DN, x_dn)
        own[k, 1, 0] = own[k, 1, 0] + part_in[k, 1, 0].astype(F32)
        own[k, 3, 1] = own[k, 3, 1] + part_in[k, 3, 1].astype(F32)
        own[k, 0] = own[k, 0] + part_in[k, 0].astype(F32)

    def relay_x(k):
        copies[k]["xa_up"].wait_recv()
        xc_send[k, 0] = (own[k, 1, 0] + xa_recv[k, 0].astype(F32)).astype(BF16)
        copies[k]["xc_up"] = send(xc_send.at[k, 0], xc_recv.at[k, 0], k, XC_UP, x_up)
        copies[k]["xa_dn"].wait_recv()
        xc_send[k, 1] = (own[k, 3, 1] + xa_recv[k, 1].astype(F32)).astype(BF16)
        copies[k]["xc_dn"] = send(xc_send.at[k, 1], xc_recv.at[k, 1], k, XC_DN, x_dn)

    def hop_y(k):
        for name in ("xb_up", "xb_dn", "xc_up", "xc_dn"):
            copies[k][name].wait_recv()
        y_send[k, 0] = (own[k, 0, 0, 1] + xb_recv[k, 1, 1].astype(F32) + xc_recv[k, 0, 1].astype(F32)).astype(BF16)
        y_send[k, 1] = (own[k, 0, 1, 1] + xb_recv[k, 0, 1].astype(F32) + xc_recv[k, 1, 1].astype(F32)).astype(BF16)
        copies[k]["y"] = send(y_send.at[k], y_recv.at[k], k, YLO, to_ylo)
        own[k, 0, 0, 0] = own[k, 0, 0, 0] + xb_recv[k, 1, 0].astype(F32) + xc_recv[k, 0, 0].astype(F32)
        own[k, 0, 1, 0] = own[k, 0, 1, 0] + xb_recv[k, 0, 0].astype(F32) + xc_recv[k, 1, 0].astype(F32)

    def prepare():
        grid_v = row_offsets[r] + place
        start = facet_offsets[facet_order[c], 1]
        block = 2 * ((z + iota(wide, 0) // 2) % 8) + (yhi + iota(wide, 0)) % 2
        twist = wave(grid_v * ((start + JB * block) & (NG - 1)))
        twist_re[...] = twist[0] * SECOND_SCALE
        twist_im[...] = twist[1] * SECOND_SCALE
        shape = (32, JB)
        coarse = wave((row_offsets[r] + 32 * iota(shape, 0)) * iota(shape, 1))
        small = wave(iota(shape, 0) * iota(shape, 1))
        for v in range(32):
            re, im = times((coarse[0][v : v + 1], coarse[1][v : v + 1]), small)
            re, im = re.astype(BF16), im.astype(BF16)
            fine[32 * v : 32 * v + 32, :JB] = re
            fine[32 * v : 32 * v + 32, JB:] = im
            fine[M + 32 * v : M + 32 * v + 32, :JB] = -im
            fine[M + 32 * v : M + 32 * v + 32, JB:] = re

    def second(k):
        copies[k]["y"].wait_recv()
        columns = (own[k, 0, 0, 0] + y_recv[k, 0].astype(F32), own[k, 0, 1, 0] + y_recv[k, 1].astype(F32))
        for b in range(NF):
            re, im = times(columns, (twist_re[b : b + 1, :], twist_im[b : b + 1, :]))
            left[b, :, :M] = re.astype(BF16)
            left[b, :, M:] = im.astype(BF16)
        image[k] = jnp.dot(
            left[...].reshape(NF * CH, 2 * M), fine[...], preferred_element_type=F32
        ).reshape(8, 2, CH, 2 * JB)
        z_send[k, 0, 0, :, :, :JB] = image[k, 4, :, :, :JB].astype(BF16)
        z_send[k, 1, 0, :, :, JB:] = image[k, 4, :, :, JB:].astype(BF16)
        copies[k]["up0"] = send(
            z_send.at[k, 0, 0, :, :, pl.ds(0, JB)], z_recv.at[k, 0, 0, :, :, pl.ds(0, JB)], k, ZUP, z_up
        )
        copies[k]["dn0"] = send(
            z_send.at[k, 1, 0, :, :, pl.ds(JB, JB)], z_recv.at[k, 1, 0, :, :, pl.ds(JB, JB)], k, ZDN, z_dn
        )

    def relay_z(k, step):
        for way, name, peer, at, index, half in (
            (0, "up", z_up, 4 - step, ZUP, slice(0, JB)),
            (1, "dn", z_dn, 4 + step, ZDN, slice(JB, 2 * JB)),
        ):
            copies[k][f"{name}{step - 1}"].wait_recv()
            if step == 1:
                other = slice(JB, 2 * JB) if way == 0 else slice(0, JB)
                z_send[k, way, step, :, :, half] = (
                    image[k, at, :, :, half] + z_recv[k, way, 0, :, :, half].astype(F32)
                ).astype(BF16)
                z_send[k, way, step, :, :, other] = image[k, at, :, :, other].astype(BF16)
            else:
                z_send[k, way, step] = (image[k, at] + z_recv[k, way, step - 1].astype(F32)).astype(BF16)
            copies[k][f"{name}{step}"] = send(
                z_send.at[k, way, step], z_recv.at[k, way, step], k, index + step, peer
            )

    def hop_h(k):
        copies[k]["up3"].wait_recv()
        copies[k]["dn3"].wait_recv()
        total = image[k, 0] + z_recv[k, 0, 3].astype(F32) + z_recv[k, 1, 3].astype(F32)
        h_send[k] = total[1].astype(BF16)
        copies[k]["h"] = send(h_send.at[k], h_recv.at[k], k, YHI, to_yhi)
        image[k, 0, 0] = total[0]

    column = (r * JB + iota((CH, JB), 1)).astype(F32)
    beam = 1.0 - BEAM_SLOPE * (column + 0.5) / FS

    def finish(k):
        copies[k]["h"].wait_recv()
        total = image[k, 0, 0] + h_recv[k].astype(F32)
        re, im = total[:, :JB] / beam, total[:, JB:] / beam
        out[0, 0, CH * k : CH * k + CH, :] = re
        out[0, 1, CH * k : CH * k + CH, :] = im
        power = re * re + im * im
        power = jnp.maximum(power[:8], power[8:])
        power = jnp.maximum(power[:, :128], power[:, 128:])
        top[...] = power if k == 0 else jnp.maximum(top[...], power)

    for load in loads:
        load.wait()
    for name, k in ORDER:
        if name == "first":
            first(k)
        elif name == "spread":
            spread_x(k)
        elif name == "relay":
            relay_x(k)
        elif name == "hop_y":
            hop_y(k)
        elif name == "prepare":
            prepare()
        elif name == "second":
            second(k)
        elif name.startswith("z"):
            relay_z(k, int(name[1:]))
        elif name == "hop_h":
            hop_h(k)
        elif name == "finish":
            finish(k)

    top[...] = jnp.sqrt(top[...])
    sends = []
    for step in range(1, NF):
        copy = pltpu.make_async_remote_copy(
            src_ref=top, dst_ref=tops.at[step], send_sem=top_send.at[step], recv_sem=top_recv.at[step],
            device_id=(c, (r + step) % NF), device_id_type=MESH,
        )
        copy.start()
        sends.append(copy)
    best = top[...]
    for step in range(1, NF):
        sends[step - 1].wait_recv()
        best = jnp.maximum(best, tops[step])
    peak[0] = jnp.max(best)
    for copy in started + sends:
        copy.wait_send()


ORDER = (
    ("first", 0), ("spread", 0),
    ("first", 1), ("spread", 1), ("relay", 0),
    ("first", 2), ("spread", 2), ("hop_y", 0), ("relay", 1),
    ("first", 3), ("spread", 3), ("prepare", 0), ("second", 0), ("hop_y", 1), ("relay", 2),
    ("z1", 0), ("second", 1), ("z2", 0), ("hop_y", 2), ("relay", 3), ("z1", 1), ("z3", 0),
    ("second", 2), ("hop_h", 0), ("z2", 1), ("hop_y", 3), ("z1", 2), ("z3", 1), ("finish", 0),
    ("second", 3), ("hop_h", 1), ("z2", 2), ("z1", 3), ("z3", 2), ("finish", 1), ("z2", 3), ("hop_h", 2),
    ("z3", 3), ("finish", 2), ("hop_h", 3), ("finish", 3),
)


def local(visibilities, col_offsets, row_offsets, facet_offsets, facet_order, vis_counts):
    vmem, smem = pltpu.VMEM, pltpu.SMEM
    scratch = [
        vmem((2, M, M), BF16),
        vmem((2, 4, 2, 2, CH, 2 * M), BF16),
        vmem((CH, M), F32), vmem((CH, M), F32),
        vmem((NCH, 4, 2, 2, CH, M), BF16),
        vmem((NCH, 4, 2, 2, CH, M), BF16),
        vmem((NCH, 4, 2, 2, CH, M), F32),
        *[vmem((NCH, 2, 2, CH, M), BF16) for _ in range(6)],
        vmem((NCH, 2, CH, M), BF16), vmem((NCH, 2, CH, M), BF16),
        vmem((NF, M), F32), vmem((NF, M), F32),
        vmem((NF, CH, 2 * M), BF16),
        vmem((2 * M, 2 * JB), BF16),
        vmem((NCH, 8, 2, CH, 2 * JB), F32),
        vmem((NCH, 2, 4, 2, CH, 2 * JB), BF16), vmem((NCH, 2, 4, 2, CH, 2 * JB), BF16),
        vmem((NCH, CH, 2 * JB), BF16), vmem((NCH, CH, 2 * JB), BF16),
        vmem((8, 128), F32), vmem((NF, 8, 128), F32),
        pltpu.SemaphoreType.DMA((2,)),
        pltpu.SemaphoreType.DMA((NCH, COPIES)), pltpu.SemaphoreType.DMA((NCH, COPIES)),
        pltpu.SemaphoreType.DMA((NF,)), pltpu.SemaphoreType.DMA((NF,)),
    ]
    return pl.pallas_call(
        body,
        out_shape=(jax.ShapeDtypeStruct((1, 2, FR, JB), F32), jax.ShapeDtypeStruct((1,), F32)),
        in_specs=[pl.BlockSpec(memory_space=pl.ANY)] + [pl.BlockSpec(memory_space=smem)] * 5,
        out_specs=(pl.BlockSpec(memory_space=vmem), pl.BlockSpec(memory_space=smem)),
        scratch_shapes=scratch,
        compiler_params=pltpu.CompilerParams(
            collective_id=0, has_side_effects=True, vmem_limit_bytes=56 * 1024 * 1024
        ),
        name="image_step",
    )(visibilities, col_offsets, row_offsets, facet_offsets, facet_order, vis_counts)


def solution(mesh):
    in_specs = (P(None, "col", "row"), P("col"), P(), P(), P(), P("col", "row"))
    out_specs = (P("col", None, None, "row"), P("col"))
    return jax.shard_map(local, mesh=mesh, in_specs=in_specs, out_specs=out_specs, check_vma=False)
```

```python
import math

import jax
import jax.numpy as jnp
from jax import lax
from jax.experimental import pallas as pl
from jax.experimental.pallas import tpu as pltpu
from jax.sharding import PartitionSpec as P

MESH = pl.DeviceIdType.MESH
F32, BF16, I32 = jnp.float32, jnp.bfloat16, jnp.int32

M = 1024
FS = 4096
NG = 16384
FR = 64
NF = 16
CH = 16
NCH = FR // CH
JB = FS // NF
TWO_PI = 2.0 * math.pi
BEAM_SLOPE = 0.66
FIRST_SCALE = 1.0 / math.sqrt(NG)
SECOND_SCALE = 0.5 / math.sqrt(NG)

LA = 640
LB = M - LA

NAMES = (
    "core", "xa_up", "xa_dn", "xb_up", "xb_dn", "xc_up", "xc_dn", "y",
    "yb", "ua_up", "ua_dn", "ub_up", "ub_dn", "uc_up", "uc_dn",
    "z3_up", "z3_dn", "z4_up", "z4_dn", "z1_up", "z1_dn", "z2_up", "z2_dn", "h",
)


def wave(exponent):
    angle = (exponent & (NG - 1)).astype(F32) * (TWO_PI / NG)
    return jnp.cos(angle), jnp.sin(angle)


def times(a, b):
    return a[0] * b[0] - a[1] * b[1], a[0] * b[1] + a[1] * b[0]


def iota(shape, dim):
    return lax.broadcasted_iota(I32, shape, dim)


def column_of(scalars, shape):
    row = iota(shape, 0)
    picked = jnp.zeros(shape, I32)
    for index, value in enumerate(scalars):
        picked = jnp.where(row == index, value, picked)
    return picked


def body(
    vis, col_offsets, row_offsets, facet_offsets, facet_order, vis_counts,
    out, peak,
    grid, table, unit_re, unit_im, part, part_in, own,
    xa_send, xb_send, xc_send, xa_recv, xb_recv, xc_recv, y_send, y_recv,
    yb_send, yb_recv, ua_send, ub_send, uc_send, ua_recv, ub_recv, uc_recv,
    twist_re, twist_im, left, fine, image, z_send, z_recv, z4_send, z4_recv, h_send, h_recv,
    result, top, tops,
    load_sem, store_sem, send_sem, recv_sem, top_send, top_recv,
):
    c, r = lax.axis_index("col"), lax.axis_index("row")
    x, ylo, core = c // 4, (c // 2) % 2, c % 2
    z, yhi = r // 2, r % 2
    to_core = (c + 1 - 2 * core, r)
    to_ylo = (c + 2 - 4 * ylo, r)
    to_yhi = (c, r + 1 - 2 * yhi)
    x_up, x_dn = ((c + 4) % 16, r), ((c + 12) % 16, r)
    z_up, z_dn = (c, (r + 2) % 16), (c, (r + 14) % 16)
    z_up2, z_dn2 = (c, (r + 4) % 16), (c, (r + 12) % 16)
    near = (to_core, to_ylo, x_up, x_dn, z_up, z_dn, z_up2, z_dn2, to_yhi)

    loads = [pltpu.make_async_copy(vis.at[p], grid.at[p], load_sem.at[p]) for p in range(2)]
    for load in loads:
        load.start()
    barrier = pltpu.get_barrier_semaphore()
    for peer in near:
        pl.semaphore_signal(barrier, inc=1, device_id=peer, device_id_type=MESH)

    started = []
    copies = [dict() for _ in range(NCH)]

    def send(k, name, src, dst, peer):
        index = NAMES.index(name)
        copy = pltpu.make_async_remote_copy(
            src_ref=src, dst_ref=dst, send_sem=send_sem.at[k, index], recv_sem=recv_sem.at[k, index],
            device_id=peer, device_id_type=MESH,
        )
        copy.start()
        started.append(copy)
        copies[k][name] = copy

    def arrived(k, *names):
        for name in names:
            copies[k][name].wait_recv()

    slots = [
        ((x + dx) % 4) * 4 + ((ylo + dy) % 2) * 2 + (core + 1 - half) % 2
        for half in range(2) for dx in range(4) for dy in range(2)
    ]
    rows_at = [facet_offsets[0, facet_order[s]] + (FS // 2 - FR // 2) for s in slots]
    wide = (NF, M)
    place = iota(wide, 1)
    grid_u = col_offsets[0] + place
    live = (place < vis_counts[0, 0]).astype(F32) * FIRST_SCALE
    slot_rows = column_of(rows_at, wide)
    unit = wave(grid_u * iota(wide, 0))
    unit_re[...], unit_im[...] = unit

    def build(k):
        base = wave(grid_u * ((slot_rows + CH * k) & (NG - 1)))
        base = (base[0] * live, base[1] * live)
        for half in range(2):
            for dx in range(4):
                for dy in range(2):
                    s = half * 8 + dx * 2 + dy
                    re, im = times((base[0][s : s + 1], base[1][s : s + 1]), (unit_re[...], unit_im[...]))
                    re, im = re.astype(BF16), im.astype(BF16)
                    table[half, dx, 0, dy, :, :M] = re
                    table[half, dx, 0, dy, :, M:] = -im
                    table[half, dx, 1, dy, :, :M] = im
                    table[half, dx, 1, dy, :, M:] = re

    def multiply(half):
        return jnp.dot(
            table[half].reshape(16 * CH, 2 * M), grid[...].reshape(2 * M, M), preferred_element_type=F32
        ).reshape(4, 2, 2, CH, M)

    def first_p(k):
        build(k)
        if k == 0:
            for load in loads:
                load.wait()
        part[k] = multiply(0).astype(BF16)
        if k == 0:
            pl.semaphore_wait(barrier, len(near))
        send(k, "core", part.at[k], part_in.at[k], to_core)

    def first_o(k):
        own[k] = multiply(1)

    A, B = slice(0, LA), slice(LA, M)

    def spread(k):
        arrived(k, "core")

        def both(dx, part_of, dy, lanes):
            return own[k, dx, part_of, dy, :, lanes] + part_in[k, dx, part_of, dy, :, lanes].astype(F32)

        def both_rows(dx, part_of):
            return own[k, dx, part_of, :, :, A] + part_in[k, dx, part_of, :, :, A].astype(F32)

        xa_send[k, 0] = both_rows(2, 0).astype(BF16)
        send(k, "xa_up", xa_send.at[k, 0], xa_recv.at[k, 0], x_up)
        xa_send[k, 1] = both_rows(2, 1).astype(BF16)
        send(k, "xa_dn", xa_send.at[k, 1], xa_recv.at[k, 1], x_dn)
        for dx in range(4):
            for q in range(2):
                yb_send[k, dx, q] = both(dx, q, 1, B).astype(BF16)
        send(k, "yb", yb_send.at[k], yb_recv.at[k], to_ylo)
        xb_send[k, 0] = both_rows(1, 1).astype(BF16)
        send(k, "xb_up", xb_send.at[k, 0], xb_recv.at[k, 0], x_up)
        xb_send[k, 1] = both_rows(3, 0).astype(BF16)
        send(k, "xb_dn", xb_send.at[k, 1], xb_recv.at[k, 1], x_dn)
        own[k, 1, 0, :, :, A] = both_rows(1, 0)
        own[k, 3, 1, :, :, A] = both_rows(3, 1)
        own[k, 0, 0, :, :, A] = both_rows(0, 0)
        own[k, 0, 1, :, :, A] = both_rows(0, 1)
        for dx in range(4):
            for q in range(2):
                own[k, dx, q, 0, :, B] = both(dx, q, 0, B)

    def relay_a(k):
        arrived(k, "xa_up")
        xc_send[k, 0] = (own[k, 1, 0, :, :, A] + xa_recv[k, 0].astype(F32)).astype(BF16)
        send(k, "xc_up", xc_send.at[k, 0], xc_recv.at[k, 0], x_up)
        arrived(k, "xa_dn")
        xc_send[k, 1] = (own[k, 3, 1, :, :, A] + xa_recv[k, 1].astype(F32)).astype(BF16)
        send(k, "xc_dn", xc_send.at[k, 1], xc_recv.at[k, 1], x_dn)

    def relay_b(k):
        arrived(k, "yb")

        def both(dx, q):
            return own[k, dx, q, 0, :, B] + yb_recv[k, dx, q].astype(F32)

        ua_send[k, 0] = both(2, 0).astype(BF16)
        send(k, "ua_up", ua_send.at[k, 0], ua_recv.at[k, 0], x_up)
        ua_send[k, 1] = both(2, 1).astype(BF16)
        send(k, "ua_dn", ua_send.at[k, 1], ua_recv.at[k, 1], x_dn)
        ub_send[k, 0] = both(1, 1).astype(BF16)
        send(k, "ub_up", ub_send.at[k, 0], ub_recv.at[k, 0], x_up)
        ub_send[k, 1] = both(3, 0).astype(BF16)
        send(k, "ub_dn", ub_send.at[k, 1], ub_recv.at[k, 1], x_dn)
        for dx, q in ((1, 0), (3, 1), (0, 0), (0, 1)):
            own[k, dx, q, 0, :, B] = both(dx, q)

    def hop_a(k):
        arrived(k, "xb_up", "xb_dn", "xc_up", "xc_dn")
        for q in range(2):
            y_send[k, q] = (
                own[k, 0, q, 1, :, A] + xb_recv[k, 1 - q, 1].astype(F32) + xc_recv[k, q, 1].astype(F32)
            ).astype(BF16)
        send(k, "y", y_send.at[k], y_recv.at[k], to_ylo)
        for q in range(2):
            own[k, 0, q, 0, :, A] = (
                own[k, 0, q, 0, :, A] + xb_recv[k, 1 - q, 0].astype(F32) + xc_recv[k, q, 0].astype(F32)
            )

    def hop_b(k):
        arrived(k, "ua_up")
        uc_send[k, 0] = (own[k, 1, 0, 0, :, B] + ua_recv[k, 0].astype(F32)).astype(BF16)
        send(k, "uc_up", uc_send.at[k, 0], uc_recv.at[k, 0], x_up)
        arrived(k, "ua_dn")
        uc_send[k, 1] = (own[k, 3, 1, 0, :, B] + ua_recv[k, 1].astype(F32)).astype(BF16)
        send(k, "uc_dn", uc_send.at[k, 1], uc_recv.at[k, 1], x_dn)

    def prepare(k):
        grid_v = row_offsets[r] + place
        start = facet_offsets[1, facet_order[c]]
        block = 2 * ((z + iota(wide, 0) // 2) % 8) + (yhi + iota(wide, 0)) % 2
        twist = wave(grid_v * ((start + JB * block) & (NG - 1)))
        twist_re[...] = twist[0] * SECOND_SCALE
        twist_im[...] = twist[1] * SECOND_SCALE
        shape = (32, JB)
        coarse = wave((row_offsets[r] + 32 * iota(shape, 0)) * iota(shape, 1))
        small = wave(iota(shape, 0) * iota(shape, 1))
        for v in range(32):
            re, im = times((coarse[0][v : v + 1], coarse[1][v : v + 1]), small)
            re, im = re.astype(BF16), im.astype(BF16)
            fine[32 * v : 32 * v + 32, :JB] = re
            fine[32 * v : 32 * v + 32, JB:] = im
            fine[M + 32 * v : M + 32 * v + 32, :JB] = -im
            fine[M + 32 * v : M + 32 * v + 32, JB:] = re

    UP, DN = slice(0, JB), slice(JB, 2 * JB)

    def second(k):
        arrived(k, "ub_up", "ub_dn", "uc_up", "uc_dn")
        for q in range(2):
            own[k, 0, q, 0, :, B] = (
                own[k, 0, q, 0, :, B] + ub_recv[k, 1 - q].astype(F32) + uc_recv[k, q].astype(F32)
            )
        arrived(k, "y")
        for q in range(2):
            own[k, 0, q, 0, :, A] = own[k, 0, q, 0, :, A] + y_recv[k, q].astype(F32)
        columns = (own[k, 0, 0, 0], own[k, 0, 1, 0])
        for b in range(NF):
            re, im = times(columns, (twist_re[b : b + 1, :], twist_im[b : b + 1, :]))
            left[b, :, :M] = re.astype(BF16)
            left[b, :, M:] = im.astype(BF16)
        image[k] = jnp.dot(
            left[...].reshape(NF * CH, 2 * M), fine[...], preferred_element_type=F32
        ).reshape(8, 2, CH, 2 * JB)
        for way, lanes, name, peer in ((0, UP, "z4_up", z_up2), (1, DN, "z4_dn", z_dn2)):
            z4_send[k, way] = image[k, 4, :, :, lanes].astype(BF16)
            send(k, name, z4_send.at[k, way], z4_recv.at[k, way], peer)
        for way, at, name, peer in (
            (0, 3, "z3_up", z_up), (1, 5, "z3_dn", z_dn), (0, 1, "z1_up", z_up), (1, 7, "z1_dn", z_dn),
        ):
            slot = 0 if name.startswith("z3") else 1
            z_send[k, way, slot] = image[k, at].astype(BF16)
            send(k, name, z_send.at[k, way, slot], z_recv.at[k, way, slot], peer)

    def relay_z(k):
        for way, at, up_or_dn, lanes, rest, peer in ((0, 2, "up", UP, DN, z_up2), (1, 6, "dn", DN, UP, z_dn2)):
            arrived(k, f"z3_{up_or_dn}", f"z4_{up_or_dn}")
            z_send[k, way, 2, :, :, lanes] = (
                image[k, at, :, :, lanes] + z_recv[k, way, 0, :, :, lanes].astype(F32) + z4_recv[k, way].astype(F32)
            ).astype(BF16)
            z_send[k, way, 2, :, :, rest] = (
                image[k, at, :, :, rest] + z_recv[k, way, 0, :, :, rest].astype(F32)
            ).astype(BF16)
            send(k, f"z2_{up_or_dn}", z_send.at[k, way, 2], z_recv.at[k, way, 2], peer)

    def hop_h(k):
        arrived(k, "z1_up", "z1_dn", "z2_up", "z2_dn")
        total = image[k, 0]
        for way in range(2):
            for slot in (1, 2):
                total = total + z_recv[k, way, slot].astype(F32)
        h_send[k] = total[1].astype(BF16)
        send(k, "h", h_send.at[k], h_recv.at[k], to_yhi)
        image[k, 0, 0] = total[0]

    stores = []

    def finish(k):
        column = (r * JB + iota((CH, JB), 1)).astype(F32)
        beam = 1.0 - BEAM_SLOPE * (column + 0.5) / FS
        arrived(k, "h")
        total = image[k, 0, 0] + h_recv[k].astype(F32)
        re, im = total[:, :JB] / beam, total[:, JB:] / beam
        rows = slice(CH * k, CH * k + CH)
        result[0, rows, :] = re
        result[1, rows, :] = im
        store = pltpu.make_async_copy(
            result.at[:, pl.ds(CH * k, CH), :], out.at[0, :, pl.ds(CH * k, CH), :], store_sem.at[k]
        )
        store.start()
        stores.append(store)
        power = re * re + im * im
        power = jnp.maximum(power[:8], power[8:])
        power = jnp.maximum(power[:, :128], power[:, 128:])
        top[...] = power if k == ORDER_FIRST else jnp.maximum(top[...], power)

    steps = {
        "first_p": first_p, "first_o": first_o, "spread": spread, "relay_a": relay_a, "relay_b": relay_b,
        "hop_a": hop_a, "hop_b": hop_b, "prepare": prepare, "second": second, "relay_z": relay_z,
        "hop_h": hop_h, "finish": finish,
    }
    for name, k in ORDER:
        with jax.named_scope(f"{name}_{k}"):
            steps[name](k)

    with jax.named_scope("peak"):
        sends = []
        for step in (8, 7, 9, 6, 10, 5, 11, 4, 12, 3, 13, 2, 14, 1, 15):
            copy = pltpu.make_async_remote_copy(
                src_ref=top, dst_ref=tops.at[step], send_sem=top_send.at[step], recv_sem=top_recv.at[step],
                device_id=(c, (r + step) % NF), device_id_type=MESH,
            )
            copy.start()
            sends.append(copy)
        best = top[...]
        for step in range(1, NF):
            sends[step - 1].wait_recv()
        for step in range(1, NF):
            best = jnp.maximum(best, tops[step])
        peak[0] = jnp.max(jnp.sqrt(best))
    with jax.named_scope("drain"):
        for store in stores:
            store.wait()
        for copy in started + sends:
            copy.wait_send()


ORDER = (
    ("first_p", 0), ("first_o", 0), ("first_p", 1), ("spread", 0), ("first_o", 1),
    ("spread", 1), ("first_p", 2), ("relay_a", 0), ("first_o", 2), ("relay_b", 0),
    ("relay_a", 1), ("spread", 2), ("first_p", 3), ("hop_a", 0), ("relay_b", 1),
    ("hop_b", 0), ("prepare", 0), ("hop_a", 1), ("first_o", 3), ("spread", 3),
    ("relay_a", 2), ("relay_b", 2), ("hop_b", 1), ("second", 0), ("relay_a", 3),
    ("relay_b", 3), ("hop_a", 2), ("hop_b", 2), ("relay_z", 0), ("second", 1),
    ("hop_a", 3), ("hop_b", 3), ("second", 2), ("second", 3), ("hop_h", 0),
    ("relay_z", 1), ("relay_z", 2), ("finish", 0), ("relay_z", 3), ("hop_h", 1),
    ("hop_h", 2), ("hop_h", 3), ("finish", 1), ("finish", 2), ("finish", 3),
)
ORDER_FIRST = 0


def local(visibilities, col_offsets, row_offsets, facet_offsets, facet_order, vis_counts):
    vmem, smem = pltpu.VMEM, pltpu.SMEM
    scratch = [
        vmem((2, M, M), BF16),
        vmem((2, 4, 2, 2, CH, 2 * M), BF16),
        vmem((CH, M), F32), vmem((CH, M), F32),
        vmem((NCH, 4, 2, 2, CH, M), BF16),
        vmem((NCH, 4, 2, 2, CH, M), BF16),
        vmem((NCH, 4, 2, 2, CH, M), F32),
        *[vmem((NCH, 2, 2, CH, LA), BF16) for _ in range(6)],
        vmem((NCH, 2, CH, LA), BF16), vmem((NCH, 2, CH, LA), BF16),
        vmem((NCH, 4, 2, CH, LB), BF16), vmem((NCH, 4, 2, CH, LB), BF16),
        *[vmem((NCH, 2, CH, LB), BF16) for _ in range(6)],
        vmem((NF, M), F32), vmem((NF, M), F32),
        vmem((NF, CH, 2 * M), BF16),
        vmem((2 * M, 2 * JB), BF16),
        vmem((NCH, 8, 2, CH, 2 * JB), F32),
        vmem((NCH, 2, 3, 2, CH, 2 * JB), BF16), vmem((NCH, 2, 3, 2, CH, 2 * JB), BF16),
        vmem((NCH, 2, 2, CH, JB), BF16), vmem((NCH, 2, 2, CH, JB), BF16),
        vmem((NCH, CH, 2 * JB), BF16), vmem((NCH, CH, 2 * JB), BF16),
        vmem((2, FR, JB), F32),
        vmem((8, 128), F32), vmem((NF, 8, 128), F32),
        pltpu.SemaphoreType.DMA((2,)), pltpu.SemaphoreType.DMA((NCH,)),
        pltpu.SemaphoreType.DMA((NCH, len(NAMES))), pltpu.SemaphoreType.DMA((NCH, len(NAMES))),
        pltpu.SemaphoreType.DMA((NF,)), pltpu.SemaphoreType.DMA((NF,)),
    ]
    return pl.pallas_call(
        body,
        out_shape=(jax.ShapeDtypeStruct((1, 2, FR, JB), F32), jax.ShapeDtypeStruct((1,), F32)),
        in_specs=[pl.BlockSpec(memory_space=pl.ANY)] + [pl.BlockSpec(memory_space=smem)] * 5,
        out_specs=(pl.BlockSpec(memory_space=pl.ANY), pl.BlockSpec(memory_space=smem)),
        scratch_shapes=scratch,
        compiler_params=pltpu.CompilerParams(
            collective_id=0, has_side_effects=True, vmem_limit_bytes=56 * 1024 * 1024
        ),
        name="image_step",
    )(visibilities, col_offsets, row_offsets, facet_offsets.T, facet_order, vis_counts)


def solution(mesh):
    in_specs = (P(None, "col", "row"), P("col"), P(), P(), P(), P("col", "row"))
    out_specs = (P("col", None, None, "row"), P("col"))
    return jax.shard_map(local, mesh=mesh, in_specs=in_specs, out_specs=out_specs, check_vma=False)
```

```python
import math

import jax
import jax.numpy as jnp
from jax import lax
from jax.experimental import pallas as pl
from jax.experimental.pallas import tpu as pltpu
from jax.sharding import PartitionSpec as P

MESH = pl.DeviceIdType.MESH
F32, BF16, I32 = jnp.float32, jnp.bfloat16, jnp.int32

M = 1024
FS = 4096
NG = 16384
FR = 64
NF = 16
CH = 8
NCH = FR // CH
TR = 2 * CH
JB = FS // NF
TWO_PI = 2.0 * math.pi
BEAM_SLOPE = 0.66
FIRST_SCALE = 1.0 / math.sqrt(NG)
SECOND_SCALE = 0.5 / math.sqrt(NG)

LA = 768
LB = M - LA
UA, UB = LA // 2, LB // 2

KINDS = ("core", "xa", "xr", "y", "yb", "ua", "ur", "zs", "zd", "h")


def wave(exponent):
    angle = (exponent & (NG - 1)).astype(F32) * (TWO_PI / NG)
    return jnp.cos(angle), jnp.sin(angle)


def times(a, b):
    return a[0] * b[0] - a[1] * b[1], a[0] * b[1] + a[1] * b[0]


def iota(shape, dim):
    return lax.broadcasted_iota(I32, shape, dim)


def column_of(scalars, shape):
    row = iota(shape, 0)
    picked = jnp.zeros(shape, I32)
    for index, value in enumerate(scalars):
        picked = jnp.where(row == index, value, picked)
    return picked


def body(
    vis, col_offsets, row_offsets, facet_offsets, facet_order, vis_counts,
    out, peak,
    grid, table, unit_re, unit_im, part, part_in, own,
    xa_send, xa_recv, xr_send, xr_recv, y_send, y_recv,
    yb_send, yb_recv, ua_send, ua_recv, ur_send, ur_recv,
    twist_re, twist_im, left, fine, image, zs_send, zs_recv, zd_send, zd_recv, h_send, h_recv,
    top, tops,
    load_sem, send_sem, recv_sem, top_send, top_recv,
):
    c, r = lax.axis_index("col"), lax.axis_index("row")
    x, ylo, core = c // 4, (c // 2) % 2, c % 2
    z, yhi = r // 2, r % 2
    to_core = (c + 1 - 2 * core, r)
    to_ylo = (c + 2 - 4 * ylo, r)
    to_yhi = (c, r + 1 - 2 * yhi)
    x_up, x_dn = ((c + 4) % 16, r), ((c + 12) % 16, r)
    z_up, z_dn = (c, (r + 2) % 16), (c, (r + 14) % 16)
    z_up2, z_dn2 = (c, (r + 4) % 16), (c, (r + 12) % 16)
    near = (to_core, to_ylo, x_up, x_dn, z_up, z_dn, z_up2, z_dn2, to_yhi)

    for p in range(2):
        for q in range(LOADS):
            rows = pl.ds(q * (M // LOADS), M // LOADS)
            pltpu.make_async_copy(vis.at[p, rows], grid.at[p, rows], load_sem).start()
    barrier = pltpu.get_barrier_semaphore()
    for peer in near:
        pl.semaphore_signal(barrier, inc=1, device_id=peer, device_id_type=MESH)

    def send(k, kind, src, dst, peer):
        index = KINDS.index(kind)
        pltpu.make_async_remote_copy(
            src_ref=src, dst_ref=dst, send_sem=send_sem.at[index], recv_sem=recv_sem.at[k, index],
            device_id=peer, device_id_type=MESH,
        ).start()

    buffers = {
        "core": (part, part_in), "xa": (xa_send, xa_recv), "xr": (xr_send, xr_recv), "y": (y_send, y_recv),
        "yb": (yb_send, yb_recv), "ua": (ua_send, ua_recv), "ur": (ur_send, ur_recv), "zs": (zs_send, zs_recv),
        "zd": (zd_send, zd_recv), "h": (h_send, h_recv),
    }

    def arrived(k, kind):
        index, (src, dst) = KINDS.index(kind), buffers[kind]
        pltpu.make_async_remote_copy(
            src_ref=src.at[k], dst_ref=dst.at[k], send_sem=send_sem.at[index], recv_sem=recv_sem.at[k, index],
            device_id=to_core, device_id_type=MESH,
        ).wait_recv()

    slots = [
        ((x + dx) % 4) * 4 + ((ylo + dy) % 2) * 2 + (core + 1 - half) % 2
        for half in range(2) for dx in range(4) for dy in range(2)
    ]
    rows_at = [facet_offsets[0, facet_order[s]] + (FS // 2 - FR // 2) for s in slots]
    wide = (NF, M)
    place = iota(wide, 1)
    grid_u = col_offsets[0] + place
    live = (place < vis_counts[0, 0]).astype(F32) * FIRST_SCALE
    slot_rows = column_of(rows_at, wide)
    unit = wave(grid_u[:CH] * iota((CH, M), 0))
    unit_re[...], unit_im[...] = unit

    def first(k):
        base = wave(grid_u * ((slot_rows + CH * k) & (NG - 1)))
        base = (base[0] * live, base[1] * live)
        for s in range(NF):
            re, im = times((base[0][s : s + 1], base[1][s : s + 1]), (unit_re[...], unit_im[...]))
            table[s, :, :M] = jnp.concatenate([re, im], axis=0).astype(BF16)
            table[s, :, M:] = jnp.concatenate([-im, re], axis=0).astype(BF16)
        if k == 0:
            pltpu.make_async_copy(vis, grid, load_sem).wait()
        product = jnp.dot(
            table[...].reshape(NF * TR, 2 * M), grid[...].reshape(2 * M, M), preferred_element_type=F32
        ).reshape(2, 4, 2, TR, M)
        part[k] = product[0].astype(BF16)
        if k == 0:
            pl.semaphore_wait(barrier, len(near))
        send(k, "core", part.at[k], part_in.at[k], to_core)
        own[k] = product[1]

    A, B = slice(0, LA), slice(LA, M)
    A_UP, A_DN, B_UP, B_DN = slice(0, UA), slice(UA, LA), slice(LA, LA + UB), slice(LA + UB, M)
    UP_A, DN_A, UP_B, DN_B = pl.ds(0, UA), pl.ds(UA, LA - UA), pl.ds(0, UB), pl.ds(UB, LB - UB)

    def spread(k):
        arrived(k, "core")

        def both(dx, lanes, dy=slice(0, 2)):
            return own[k, dx, dy, :, lanes] + part_in[k, dx, dy, :, lanes].astype(F32)

        xa_send[k] = both(2, A).astype(BF16)
        send(k, "xa", xa_send.at[k, :, :, UP_A], xa_recv.at[k, :, :, UP_A], x_up)
        send(k, "xa", xa_send.at[k, :, :, DN_A], xa_recv.at[k, :, :, DN_A], x_dn)
        for dx in range(4):
            yb_send[k, dx] = both(dx, B, 1).astype(BF16)
        send(k, "yb", yb_send.at[k], yb_recv.at[k], to_ylo)
        xr_send[k, 0, :, :, A_DN] = both(1, A_DN).astype(BF16)
        send(k, "xr", xr_send.at[k, 0, :, :, DN_A], xr_recv.at[k, 0, :, :, DN_A], x_up)
        xr_send[k, 0, :, :, A_UP] = both(3, A_UP).astype(BF16)
        send(k, "xr", xr_send.at[k, 0, :, :, UP_A], xr_recv.at[k, 0, :, :, UP_A], x_dn)
        own[k, 1, :, :, A_UP] = both(1, A_UP)
        own[k, 3, :, :, A_DN] = both(3, A_DN)
        own[k, 0, :, :, A] = both(0, A)
        for dx in range(4):
            own[k, dx, 0, :, B] = both(dx, B, 0)

    def relay_a(k):
        arrived(k, "xa")
        xr_send[k, 1, :, :, A_UP] = (own[k, 1, :, :, A_UP] + xa_recv[k, :, :, A_UP].astype(F32)).astype(BF16)
        send(k, "xr", xr_send.at[k, 1, :, :, UP_A], xr_recv.at[k, 1, :, :, UP_A], x_up)
        xr_send[k, 1, :, :, A_DN] = (own[k, 3, :, :, A_DN] + xa_recv[k, :, :, A_DN].astype(F32)).astype(BF16)
        send(k, "xr", xr_send.at[k, 1, :, :, DN_A], xr_recv.at[k, 1, :, :, DN_A], x_dn)

    def hop_a(k):
        arrived(k, "xr")

        def summed(dy):
            return own[k, 0, dy, :, A] + xr_recv[k, 0, dy].astype(F32) + xr_recv[k, 1, dy].astype(F32)

        y_send[k] = summed(1).astype(BF16)
        send(k, "y", y_send.at[k], y_recv.at[k], to_ylo)
        own[k, 0, 0, :, A] = summed(0)

    def relay_b(k):
        arrived(k, "yb")

        def both(dx, lanes, rows):
            return own[k, dx, 0, :, lanes] + yb_recv[k, dx, :, rows].astype(F32)

        up, dn = slice(0, UB), slice(UB, LB)
        ua_send[k] = both(2, B, slice(0, LB)).astype(BF16)
        send(k, "ua", ua_send.at[k, :, UP_B], ua_recv.at[k, :, UP_B], x_up)
        send(k, "ua", ua_send.at[k, :, DN_B], ua_recv.at[k, :, DN_B], x_dn)
        ur_send[k, 0, :, dn] = both(1, B_DN, dn).astype(BF16)
        send(k, "ur", ur_send.at[k, 0, :, DN_B], ur_recv.at[k, 0, :, DN_B], x_up)
        ur_send[k, 0, :, up] = both(3, B_UP, up).astype(BF16)
        send(k, "ur", ur_send.at[k, 0, :, UP_B], ur_recv.at[k, 0, :, UP_B], x_dn)
        own[k, 1, 0, :, B_UP] = both(1, B_UP, up)
        own[k, 3, 0, :, B_DN] = both(3, B_DN, dn)
        own[k, 0, 0, :, B] = both(0, B, slice(0, LB))

    def hop_b(k):
        arrived(k, "ua")
        up, dn = slice(0, UB), slice(UB, LB)
        ur_send[k, 1, :, up] = (own[k, 1, 0, :, B_UP] + ua_recv[k, :, up].astype(F32)).astype(BF16)
        send(k, "ur", ur_send.at[k, 1, :, UP_B], ur_recv.at[k, 1, :, UP_B], x_up)
        ur_send[k, 1, :, dn] = (own[k, 3, 0, :, B_DN] + ua_recv[k, :, dn].astype(F32)).astype(BF16)
        send(k, "ur", ur_send.at[k, 1, :, DN_B], ur_recv.at[k, 1, :, DN_B], x_dn)

    def prepare(k):
        grid_v = row_offsets[r] + place
        start = facet_offsets[1, facet_order[c]]
        block = 2 * ((z + iota(wide, 0) // 2) % 8) + (yhi + iota(wide, 0)) % 2
        twist = wave(grid_v * ((start + JB * block) & (NG - 1)))
        twist_re[...] = twist[0] * SECOND_SCALE
        twist_im[...] = twist[1] * SECOND_SCALE
        shape = (32, JB)
        coarse = wave((row_offsets[r] + 32 * iota(shape, 0)) * iota(shape, 1))
        small = wave(iota(shape, 0) * iota(shape, 1))
        for v in range(32):
            re, im = times((coarse[0][v : v + 1], coarse[1][v : v + 1]), small)
            re, im = re.astype(BF16), im.astype(BF16)
            fine[32 * v : 32 * v + 32, :JB] = re
            fine[32 * v : 32 * v + 32, JB:] = im
            fine[M + 32 * v : M + 32 * v + 32, :JB] = -im
            fine[M + 32 * v : M + 32 * v + 32, JB:] = re

    def second(k):
        arrived(k, "ur")
        right = own[k, 0, 0, :, B] + ur_recv[k, 0].astype(F32) + ur_recv[k, 1].astype(F32)
        arrived(k, "y")
        columns = jnp.concatenate([own[k, 0, 0, :, A] + y_recv[k].astype(F32), right], axis=1)
        columns = (columns[:CH], columns[CH:])
        for d in range(8):
            pair = [
                times(columns, (twist_re[b : b + 1, :], twist_im[b : b + 1, :])) for b in (2 * d, 2 * d + 1)
            ]
            for q in range(2):
                left[d, :, M * q : M * q + M] = jnp.concatenate([pair[0][q], pair[1][q]], axis=0).astype(BF16)
        image[k] = jnp.dot(
            left[...].reshape(NF * CH, 2 * M), fine[...], preferred_element_type=F32
        ).reshape(8, TR, 2 * JB)
        for way, at, half, peer, peer2 in ((0, 3, 0, z_up, z_up2), (1, 5, 1, z_dn, z_dn2)):
            zs_send[k, way, 2] = image[k, 4, :, JB * half : JB * half + JB].astype(BF16)
            send(k, "zs", zs_send.at[k, way, 2], zs_recv.at[k, way, 2], peer2)
            for q in range(2):
                zs_send[k, way, q] = image[k, at, :, JB * q : JB * q + JB].astype(BF16)
            send(k, "zs", zs_send.at[k, way, pl.ds(0, 2)], zs_recv.at[k, way, pl.ds(0, 2)], peer)
        for way, at, peer in ((0, 1, z_up), (1, 7, z_dn)):
            zd_send[k, way] = image[k, at].astype(BF16)
            send(k, "zd", zd_send.at[k, way], zd_recv.at[k, way], peer)

    def relay_z(k):
        arrived(k, "zs")
        for way, at, half, peer in ((0, 2, 0, z_up2), (1, 6, 1, z_dn2)):
            for q in range(2):
                lanes = slice(JB * q, JB * q + JB)
                total = image[k, at, :, lanes] + zs_recv[k, way, q].astype(F32)
                if q == half:
                    total = total + zs_recv[k, way, 2].astype(F32)
                zd_send[k, 2 + way, :, lanes] = total.astype(BF16)
            send(k, "zd", zd_send.at[k, 2 + way], zd_recv.at[k, 2 + way], peer)

    def hop_h(k):
        arrived(k, "zd")
        total = image[k, 0]
        for way in range(4):
            total = total + zd_recv[k, way].astype(F32)
        h_send[k] = jnp.concatenate([total[CH:, :JB], total[CH:, JB:]], axis=0).astype(BF16)
        send(k, "h", h_send.at[k], h_recv.at[k], to_yhi)
        image[k, 0, :CH] = total[:CH]

    def finish(k):
        column = (r * JB + iota((CH, JB), 1)).astype(F32)
        beam = 1.0 - BEAM_SLOPE * (column + 0.5) / FS
        arrived(k, "h")
        total = h_recv[k].astype(F32)
        re = (image[k, 0, :CH, :JB] + total[:CH]) / beam
        im = (image[k, 0, :CH, JB:] + total[CH:]) / beam
        rows = slice(CH * k, CH * k + CH)
        out[0, 0, rows, :] = re
        out[0, 1, rows, :] = im
        power = re * re + im * im
        power = jnp.maximum(power[:, :128], power[:, 128:])
        top[...] = power if k == ORDER_FIRST else jnp.maximum(top[...], power)

    steps = {
        "first": first, "spread": spread, "relay_a": relay_a, "relay_b": relay_b, "hop_a": hop_a, "hop_b": hop_b,
        "prepare": prepare, "second": second, "relay_z": relay_z, "hop_h": hop_h, "finish": finish,
    }
    for name, k in ORDER:
        with jax.named_scope(f"{name}_{k}"):
            steps[name](k)

    with jax.named_scope("peak"):
        for step in (8, 7, 9, 6, 10, 5, 11, 4, 12, 3, 13, 2, 14, 1, 15):
            pltpu.make_async_remote_copy(
                src_ref=top, dst_ref=tops.at[step - 1], send_sem=top_send, recv_sem=top_recv,
                device_id=(c, (r + step) % NF), device_id_type=MESH,
            ).start()
        all_tops = pltpu.make_async_remote_copy(
            src_ref=tops, dst_ref=tops, send_sem=top_send, recv_sem=top_recv, device_id=to_core, device_id_type=MESH
        )
        all_tops.wait_recv()
        best = top[...]
        for step in range(NF - 1):
            best = jnp.maximum(best, tops[step])
        peak[...] = jnp.full((8, 128), jnp.max(jnp.sqrt(best)))
    with jax.named_scope("drain"):
        all_tops.wait_send()
        for index, kind in enumerate(KINDS):
            src, dst = buffers[kind]
            pltpu.make_async_remote_copy(
                src_ref=src, dst_ref=dst, send_sem=send_sem.at[index], recv_sem=recv_sem.at[0, index],
                device_id=to_core, device_id_type=MESH,
            ).wait_send()


LOADS = 4
ORDER = (
    ("first", 0), ("first", 1), ("spread", 0), ("first", 2), ("spread", 1),
    ("first", 3), ("spread", 2), ("relay_a", 0), ("first", 4), ("relay_b", 0),
    ("relay_a", 1), ("relay_b", 1), ("spread", 3), ("first", 5), ("relay_a", 2),
    ("relay_b", 2), ("spread", 4), ("first", 6), ("hop_a", 0), ("hop_b", 0),
    ("hop_b", 1), ("hop_a", 1), ("spread", 5), ("relay_b", 3), ("first", 7),
    ("relay_a", 3), ("hop_b", 2), ("relay_b", 4), ("spread", 6), ("hop_a", 2),
    ("prepare", 0), ("relay_a", 4), ("second", 0), ("relay_a", 5), ("second", 1),
    ("spread", 7), ("hop_b", 3), ("hop_a", 3), ("relay_b", 5), ("second", 2),
    ("relay_a", 6), ("relay_b", 6), ("relay_z", 0), ("hop_b", 4), ("hop_a", 4),
    ("hop_a", 5), ("relay_a", 7), ("relay_z", 1), ("hop_b", 5), ("relay_b", 7),
    ("second", 3), ("hop_a", 6), ("hop_b", 6), ("relay_z", 2), ("second", 4),
    ("hop_a", 7), ("hop_b", 7), ("second", 5), ("second", 6), ("relay_z", 3),
    ("second", 7), ("relay_z", 5), ("relay_z", 4), ("relay_z", 6), ("relay_z", 7),
    ("hop_h", 3), ("hop_h", 5), ("hop_h", 1), ("hop_h", 4), ("hop_h", 2),
    ("hop_h", 6), ("hop_h", 0), ("hop_h", 7), ("finish", 5), ("finish", 1),
    ("finish", 3), ("finish", 6), ("finish", 0), ("finish", 2), ("finish", 4),
    ("finish", 7),
)
ORDER_FIRST = 5


def local(visibilities, col_offsets, row_offsets, facet_offsets, facet_order, vis_counts):
    vmem, smem = pltpu.VMEM, pltpu.SMEM

    def twice(*shape):
        return [vmem((NCH, *shape), BF16), vmem((NCH, *shape), BF16)]

    scratch = [
        vmem((2, M, M), BF16),
        vmem((NF, TR, 2 * M), BF16),
        vmem((CH, M), F32), vmem((CH, M), F32),
        *twice(4, 2, TR, M),
        vmem((NCH, 4, 2, TR, M), F32),
        *twice(2, TR, LA), *twice(2, 2, TR, LA), *twice(TR, LA),
        *twice(4, TR, LB), *twice(TR, LB), *twice(2, TR, LB),
        vmem((NF, M), F32), vmem((NF, M), F32),
        vmem((8, TR, 2 * M), BF16),
        vmem((2 * M, 2 * JB), BF16),
        vmem((NCH, 8, TR, 2 * JB), F32),
        *twice(2, 3, TR, JB), *twice(4, TR, 2 * JB), *twice(TR, JB),
        vmem((8, 128), F32), vmem((NF - 1, 8, 128), F32),
        pltpu.SemaphoreType.DMA,
        pltpu.SemaphoreType.DMA((len(KINDS),)), pltpu.SemaphoreType.DMA((NCH, len(KINDS))),
        pltpu.SemaphoreType.DMA, pltpu.SemaphoreType.DMA,
    ]
    images, peak = pl.pallas_call(
        body,
        out_shape=(vmem((1, 2, FR, JB), F32), vmem((8, 128), F32)),
        in_specs=[pl.BlockSpec(memory_space=pl.ANY)] + [pl.BlockSpec(memory_space=smem)] * 5,
        out_specs=(pl.BlockSpec(memory_space=vmem), pl.BlockSpec(memory_space=vmem)),
        scratch_shapes=scratch,
        compiler_params=pltpu.CompilerParams(
            collective_id=0, has_side_effects=True, vmem_limit_bytes=56 * 1024 * 1024
        ),
        name="image_step",
    )(visibilities, col_offsets, row_offsets, facet_offsets.T, facet_order, vis_counts)
    return images, peak[0, :1]


def solution(mesh):
    in_specs = (P(None, "col", "row"), P("col"), P(), P(), P(), P("col", "row"))
    out_specs = (P("col", None, None, "row"), P("col"))
    return jax.shard_map(local, mesh=mesh, in_specs=in_specs, out_specs=out_specs, check_vma=False)
```

```python
import math

import jax
import jax.numpy as jnp
from jax import lax
from jax.experimental import pallas as pl
from jax.experimental.pallas import tpu as pltpu
from jax.sharding import PartitionSpec as P

MESH = pl.DeviceIdType.MESH
F32, BF16, I32 = jnp.float32, jnp.bfloat16, jnp.int32

M = 1024
FS = 4096
NG = 16384
FR = 64
NF = 16
CH = 8
NCH = FR // CH
TR = 2 * CH
JB = FS // NF
TWO_PI = 2.0 * math.pi
BEAM_SLOPE = 0.66
FIRST_SCALE = 1.0 / math.sqrt(NG)
SECOND_SCALE = 0.5 / math.sqrt(NG)

LA = 640
LB = M - LA
UP_LANES = ((384, 128), (256, 256))
MERGED = (6, 7)

KINDS = ("core", "xa", "xr", "y", "yb", "ua", "ur", "zs", "zd", "h")


def wave(exponent):
    angle = (exponent & (NG - 1)).astype(F32) * (TWO_PI / NG)
    return jnp.cos(angle), jnp.sin(angle)


def times(a, b):
    return a[0] * b[0] - a[1] * b[1], a[0] * b[1] + a[1] * b[0]


def iota(shape, dim):
    return lax.broadcasted_iota(I32, shape, dim)


def column_of(scalars, shape):
    row = iota(shape, 0)
    picked = jnp.zeros(shape, I32)
    for index, value in enumerate(scalars):
        picked = jnp.where(row == index, value, picked)
    return picked


def body(
    vis, col_offsets, row_offsets, facet_offsets, facet_order, vis_counts,
    out, peak,
    grid, table, unit_re, unit_im, base_re, base_im, turn_re, turn_im, part, part_in, own,
    xa_send, xa_recv, xr_send, xr_recv, y_send, y_recv,
    yb_send, yb_recv, ua_send, ua_recv, ur_send, ur_recv,
    twist_re, twist_im, left, fine, image, zs_send, zs_recv, zd_send, zd_recv, zm_send, zm_recv, h_send, h_recv,
    top, tops,
    load_sem, send_sem, recv_sem, top_send, top_recv,
):
    c, r = lax.axis_index("col"), lax.axis_index("row")
    x, ylo, core = c // 4, (c // 2) % 2, c % 2
    z, yhi = r // 2, r % 2
    to_core = (c + 1 - 2 * core, r)
    to_ylo = (c + 2 - 4 * ylo, r)
    to_yhi = (c, r + 1 - 2 * yhi)
    x_up, x_dn = ((c + 4) % 16, r), ((c + 12) % 16, r)
    z_up, z_dn = (c, (r + 2) % 16), (c, (r + 14) % 16)
    z_up2, z_dn2 = (c, (r + 4) % 16), (c, (r + 12) % 16)
    across = [(c, (2 * (z + d) + 1 - yhi) % 16) for d in (1, 7, 2, 6)]
    near = (to_core, to_ylo, x_up, x_dn, z_up, z_dn, z_up2, z_dn2, to_yhi, *across)

    for p in range(2):
        for q in range(LOADS):
            rows = pl.ds(q * (M // LOADS), M // LOADS)
            pltpu.make_async_copy(vis.at[p, rows], grid.at[p, rows], load_sem).start()
    barrier = pltpu.get_barrier_semaphore()
    for peer in near:
        pl.semaphore_signal(barrier, inc=1, device_id=peer, device_id_type=MESH)

    def at(k, kind):
        if kind == "zm":
            return MERGED.index(k)
        return NOT_MERGED.index(k) if kind in ("zd", "h") else k

    def send_index(kind):
        return len(KINDS) if kind == "zm" else KINDS.index(kind)

    def send(k, kind, src, dst, peer):
        pltpu.make_async_remote_copy(
            src_ref=src, dst_ref=dst, send_sem=send_sem.at[send_index(kind)],
            recv_sem=recv_sem.at[k, KINDS.index("zd" if kind == "zm" else kind)],
            device_id=peer, device_id_type=MESH,
        ).start()

    buffers = {
        "core": (part, part_in), "xa": (xa_send, xa_recv), "xr": (xr_send, xr_recv), "y": (y_send, y_recv),
        "yb": (yb_send, yb_recv), "ua": (ua_send, ua_recv), "ur": (ur_send, ur_recv), "zs": (zs_send, zs_recv),
        "zd": (zd_send, zd_recv), "h": (h_send, h_recv), "zm": (zm_send, zm_recv),
    }

    def arrived(k, kind):
        src, dst = buffers[kind]
        pltpu.make_async_remote_copy(
            src_ref=src.at[at(k, kind)], dst_ref=dst.at[at(k, kind)], send_sem=send_sem.at[send_index(kind)],
            recv_sem=recv_sem.at[k, KINDS.index("zd" if kind == "zm" else kind)],
            device_id=to_core, device_id_type=MESH,
        ).wait_recv()

    slots = [
        ((x + dx) % 4) * 4 + ((ylo + dy) % 2) * 2 + (core + 1 - half) % 2
        for half in range(2) for dx in range(4) for dy in range(2)
    ]
    rows_at = [facet_offsets[0, facet_order[s]] + (FS // 2 - FR // 2) for s in slots]
    wide = (NF, M)
    place = iota(wide, 1)
    grid_u = col_offsets[0] + place
    live = (place < vis_counts[0, 0]).astype(F32) * FIRST_SCALE
    slot_rows = column_of(rows_at, wide)
    small = (CH, M)
    for (re, im), wave_of in (
        ((unit_re, unit_im), grid_u[:CH] * iota(small, 0)),
        ((turn_re, turn_im), grid_u[:CH] * (CH * iota(small, 0))),
        ((base_re, base_im), grid_u * (slot_rows & (NG - 1))),
    ):
        re[...], im[...] = wave(wave_of)
    base_re[...], base_im[...] = base_re[...] * live, base_im[...] * live

    def build(k):
        turn = (turn_re[k : k + 1, :], turn_im[k : k + 1, :])
        base = times((base_re[...], base_im[...]), turn) if k else (base_re[...], base_im[...])
        for s in range(NF):
            re, im = times((base[0][s : s + 1], base[1][s : s + 1]), (unit_re[...], unit_im[...]))
            table[k % 2, s, :, :M] = jnp.concatenate([re, im], axis=0).astype(BF16)
            table[k % 2, s, :, M:] = jnp.concatenate([-im, re], axis=0).astype(BF16)

    def multiply(rows):
        return jnp.dot(rows.reshape(-1, 2 * M), grid[...].reshape(2 * M, M), preferred_element_type=F32)

    def first(k):
        if k == 0:
            build(0)
            pltpu.make_async_copy(vis, grid, load_sem).wait()
            part[0] = multiply(table[0, :8]).astype(BF16).reshape(4, 2, TR, M)
            pl.semaphore_wait(barrier, len(near))
            send(k, "core", part.at[k], part_in.at[k], to_core)
            own[0] = multiply(table[0, 8:]).reshape(4, 2, TR, M)
            build(1)
            return
        product = multiply(table[k % 2]).reshape(2, 4, 2, TR, M)
        if k + 1 < NCH:
            build(k + 1)
        part[k] = product[0].astype(BF16)
        own[k] = product[1]
        send(k, "core", part.at[k], part_in.at[k], to_core)

    A, B = slice(0, LA), slice(LA, M)

    def halves(k):
        ua, ub = UP_LANES[k % 2]
        return (
            (slice(0, ua), slice(ua, LA), slice(LA, LA + ub), slice(LA + ub, M)),
            (pl.ds(0, ua), pl.ds(ua, LA - ua), pl.ds(0, ub), pl.ds(ub, LB - ub)),
        )

    def spread(k):
        (A_UP, A_DN, _, _), (UP_A, DN_A, _, _) = halves(k)
        arrived(k, "core")

        def both(dx, lanes, dy=slice(0, 2)):
            return own[k, dx, dy, :, lanes] + part_in[k, dx, dy, :, lanes].astype(F32)

        xa_send[k] = both(2, A).astype(BF16)
        send(k, "xa", xa_send.at[k, :, :, UP_A], xa_recv.at[k, :, :, UP_A], x_up)
        send(k, "xa", xa_send.at[k, :, :, DN_A], xa_recv.at[k, :, :, DN_A], x_dn)
        for dx in range(4):
            yb_send[k, dx] = both(dx, B, 1).astype(BF16)
        send(k, "yb", yb_send.at[k], yb_recv.at[k], to_ylo)
        xr_send[k, 0, :, :, A_DN] = both(1, A_DN).astype(BF16)
        send(k, "xr", xr_send.at[k, 0, :, :, DN_A], xr_recv.at[k, 0, :, :, DN_A], x_up)
        xr_send[k, 0, :, :, A_UP] = both(3, A_UP).astype(BF16)
        send(k, "xr", xr_send.at[k, 0, :, :, UP_A], xr_recv.at[k, 0, :, :, UP_A], x_dn)
        own[k, 1, :, :, A_UP] = both(1, A_UP)
        own[k, 3, :, :, A_DN] = both(3, A_DN)
        own[k, 0, :, :, A] = both(0, A)
        for dx in range(4):
            own[k, dx, 0, :, B] = both(dx, B, 0)

    def relay_a(k):
        (A_UP, A_DN, _, _), (UP_A, DN_A, _, _) = halves(k)
        arrived(k, "xa")
        xr_send[k, 1, :, :, A_UP] = (own[k, 1, :, :, A_UP] + xa_recv[k, :, :, A_UP].astype(F32)).astype(BF16)
        send(k, "xr", xr_send.at[k, 1, :, :, UP_A], xr_recv.at[k, 1, :, :, UP_A], x_up)
        xr_send[k, 1, :, :, A_DN] = (own[k, 3, :, :, A_DN] + xa_recv[k, :, :, A_DN].astype(F32)).astype(BF16)
        send(k, "xr", xr_send.at[k, 1, :, :, DN_A], xr_recv.at[k, 1, :, :, DN_A], x_dn)

    def hop_a(k):
        arrived(k, "xr")

        def summed(dy):
            return own[k, 0, dy, :, A] + xr_recv[k, 0, dy].astype(F32) + xr_recv[k, 1, dy].astype(F32)

        y_send[k] = summed(1).astype(BF16)
        send(k, "y", y_send.at[k], y_recv.at[k], to_ylo)
        own[k, 0, 0, :, A] = summed(0)

    def relay_b(k):
        (_, _, B_UP, B_DN), (_, _, UP_B, DN_B) = halves(k)
        arrived(k, "yb")

        def both(dx, lanes, rows):
            return own[k, dx, 0, :, lanes] + yb_recv[k, dx, :, rows].astype(F32)

        up, dn = slice(0, UP_LANES[k % 2][1]), slice(UP_LANES[k % 2][1], LB)
        ua_send[k] = both(2, B, slice(0, LB)).astype(BF16)
        send(k, "ua", ua_send.at[k, :, UP_B], ua_recv.at[k, :, UP_B], x_up)
        send(k, "ua", ua_send.at[k, :, DN_B], ua_recv.at[k, :, DN_B], x_dn)
        ur_send[k, 0, :, dn] = both(1, B_DN, dn).astype(BF16)
        send(k, "ur", ur_send.at[k, 0, :, DN_B], ur_recv.at[k, 0, :, DN_B], x_up)
        ur_send[k, 0, :, up] = both(3, B_UP, up).astype(BF16)
        send(k, "ur", ur_send.at[k, 0, :, UP_B], ur_recv.at[k, 0, :, UP_B], x_dn)
        own[k, 1, 0, :, B_UP] = both(1, B_UP, up)
        own[k, 3, 0, :, B_DN] = both(3, B_DN, dn)
        own[k, 0, 0, :, B] = both(0, B, slice(0, LB))

    def hop_b(k):
        (_, _, B_UP, B_DN), (_, _, UP_B, DN_B) = halves(k)
        arrived(k, "ua")
        up, dn = slice(0, UP_LANES[k % 2][1]), slice(UP_LANES[k % 2][1], LB)
        ur_send[k, 1, :, up] = (own[k, 1, 0, :, B_UP] + ua_recv[k, :, up].astype(F32)).astype(BF16)
        send(k, "ur", ur_send.at[k, 1, :, UP_B], ur_recv.at[k, 1, :, UP_B], x_up)
        ur_send[k, 1, :, dn] = (own[k, 3, 0, :, B_DN] + ua_recv[k, :, dn].astype(F32)).astype(BF16)
        send(k, "ur", ur_send.at[k, 1, :, DN_B], ur_recv.at[k, 1, :, DN_B], x_dn)

    def prepare(k):
        grid_v = row_offsets[r] + place
        start = facet_offsets[1, facet_order[c]]
        block = 2 * ((z + iota(wide, 0) // 2) % 8) + (yhi + iota(wide, 0)) % 2
        twist = wave(grid_v * ((start + JB * block) & (NG - 1)))
        twist_re[...] = twist[0] * SECOND_SCALE
        twist_im[...] = twist[1] * SECOND_SCALE
        shape = (32, JB)
        coarse = wave((row_offsets[r] + 32 * iota(shape, 0)) * iota(shape, 1))
        small = wave(iota(shape, 0) * iota(shape, 1))
        for v in range(32):
            re, im = times((coarse[0][v : v + 1], coarse[1][v : v + 1]), small)
            re, im = re.astype(BF16), im.astype(BF16)
            fine[32 * v : 32 * v + 32, :JB] = re
            fine[32 * v : 32 * v + 32, JB:] = im
            fine[M + 32 * v : M + 32 * v + 32, :JB] = -im
            fine[M + 32 * v : M + 32 * v + 32, JB:] = re

    def second(k):
        arrived(k, "ur")
        right = own[k, 0, 0, :, B] + ur_recv[k, 0].astype(F32) + ur_recv[k, 1].astype(F32)
        arrived(k, "y")
        columns = jnp.concatenate([own[k, 0, 0, :, A] + y_recv[k].astype(F32), right], axis=1)
        columns = (columns[:CH], columns[CH:])
        for d in range(8):
            pair = [
                times(columns, (twist_re[b : b + 1, :], twist_im[b : b + 1, :])) for b in (2 * d, 2 * d + 1)
            ]
            for q in range(2):
                left[d, :, M * q : M * q + M] = jnp.concatenate([pair[0][q], pair[1][q]], axis=0).astype(BF16)
        image[k] = jnp.dot(
            left[...].reshape(NF * CH, 2 * M), fine[...], preferred_element_type=F32
        ).reshape(8, TR, 2 * JB)
        for way, dz, half, peer, peer2 in ((0, 3, 0, z_up, z_up2), (1, 5, 1, z_dn, z_dn2)):
            zs_send[k, way, 2] = image[k, 4, :, JB * half : JB * half + JB].astype(BF16)
            send(k, "zs", zs_send.at[k, way, 2], zs_recv.at[k, way, 2], peer2)
            for q in range(2):
                zs_send[k, way, q] = image[k, dz, :, JB * q : JB * q + JB].astype(BF16)
            send(k, "zs", zs_send.at[k, way, pl.ds(0, 2)], zs_recv.at[k, way, pl.ds(0, 2)], peer)
        for way, dz, peer in ((0, 1, z_up), (1, 7, z_dn)):
            if k in MERGED:
                merged_sends(k, way, image[k, dz], peer)
            else:
                n = at(k, "zd")
                zd_send[n, way] = image[k, dz].astype(BF16)
                send(k, "zd", zd_send.at[n, way], zd_recv.at[n, way], peer)
        if k in MERGED:
            n = at(k, "zm")
            zm_send[n, 8] = folded(image[k, 0, CH:]).astype(BF16)
            send(k, "zm", zm_send.at[n, 8], zm_recv.at[n, 8], to_yhi)

    def folded(rows):
        return jnp.concatenate([rows[:, :JB], rows[:, JB:]], axis=0)

    def merged_sends(k, way, total, peer):
        n = at(k, "zm")
        for other, owner in ((1, across[way]), (0, peer)):
            zm_send[n, 4 * other + way] = folded(total[CH * other : CH * other + CH]).astype(BF16)
            send(k, "zm", zm_send.at[n, 4 * other + way], zm_recv.at[n, 4 * other + way], owner)

    def relay_z(k):
        arrived(k, "zs")
        for way, dz, half, peer in ((0, 2, 0, z_up2), (1, 6, 1, z_dn2)):
            total = [image[k, dz, :, JB * q : JB * q + JB] + zs_recv[k, way, q].astype(F32) for q in range(2)]
            total[half] = total[half] + zs_recv[k, way, 2].astype(F32)
            if k in MERGED:
                merged_sends(k, 2 + way, jnp.concatenate(total, axis=1), peer)
            else:
                n = at(k, "zd")
                for q in range(2):
                    zd_send[n, 2 + way, :, JB * q : JB * q + JB] = total[q].astype(BF16)
                send(k, "zd", zd_send.at[n, 2 + way], zd_recv.at[n, 2 + way], peer)

    def hop_h(k):
        arrived(k, "zd")
        total, n = image[k, 0], at(k, "zd")
        for way in range(4):
            total = total + zd_recv[n, way].astype(F32)
        h_send[n] = folded(total[CH:]).astype(BF16)
        send(k, "h", h_send.at[n], h_recv.at[n], to_yhi)
        image[k, 0, :CH] = total[:CH]

    def finish(k):
        column = (r * JB + iota((TR, JB), 1)).astype(F32)
        beam = 1.0 - BEAM_SLOPE * (column + 0.5) / FS
        total = folded(image[k, 0, :CH])
        if k in MERGED:
            arrived(k, "zm")
            for n in range(9):
                total = total + zm_recv[at(k, "zm"), n].astype(F32)
        else:
            arrived(k, "h")
            total = total + h_recv[at(k, "h")].astype(F32)
        total = total / beam
        re, im = total[:CH], total[CH:]
        rows = slice(CH * k, CH * k + CH)
        out[0, 0, rows, :] = re
        out[0, 1, rows, :] = im
        power = re * re + im * im
        power = jnp.maximum(power[:, :128], power[:, 128:])
        top[...] = power if k == ORDER_FIRST else jnp.maximum(top[...], power)

    steps = {
        "first": first, "spread": spread, "relay_a": relay_a, "relay_b": relay_b, "hop_a": hop_a, "hop_b": hop_b,
        "prepare": prepare, "second": second, "relay_z": relay_z, "hop_h": hop_h, "finish": finish,
    }
    for name, k in ORDER:
        with jax.named_scope(f"{name}_{k}"):
            steps[name](k)

    with jax.named_scope("peak"):
        for step in (8, 7, 9, 6, 10, 5, 11, 4, 12, 3, 13, 2, 14, 1, 15):
            pltpu.make_async_remote_copy(
                src_ref=top, dst_ref=tops.at[step - 1], send_sem=top_send, recv_sem=top_recv,
                device_id=(c, (r + step) % NF), device_id_type=MESH,
            ).start()
        all_tops = pltpu.make_async_remote_copy(
            src_ref=tops, dst_ref=tops, send_sem=top_send, recv_sem=top_recv, device_id=to_core, device_id_type=MESH
        )
        all_tops.wait_recv()
        best = top[...]
        for step in range(NF - 1):
            best = jnp.maximum(best, tops[step])
        peak[...] = jnp.full((8, 128), jnp.max(jnp.sqrt(best)))
    with jax.named_scope("drain"):
        all_tops.wait_send()
        for kind, (src, dst) in buffers.items():
            index = 0
            pltpu.make_async_remote_copy(
                src_ref=src, dst_ref=dst, send_sem=send_sem.at[send_index(kind)], recv_sem=recv_sem.at[0, index],
                device_id=to_core, device_id_type=MESH,
            ).wait_send()


LOADS = 4
NOT_MERGED = tuple(k for k in range(NCH) if k not in MERGED)
ORDER = (
    ("prepare", 0), ("first", 0), ("first", 1), ("spread", 0), ("first", 2),
    ("spread", 1), ("first", 3), ("spread", 2), ("relay_a", 0), ("first", 4),
    ("relay_b", 0), ("relay_a", 1), ("relay_b", 1), ("spread", 3), ("first", 5),
    ("relay_a", 2), ("relay_b", 2), ("hop_a", 0), ("hop_b", 0), ("spread", 4),
    ("first", 6), ("hop_b", 1), ("hop_a", 1), ("spread", 5), ("relay_a", 3),
    ("first", 7), ("hop_b", 2), ("hop_a", 2), ("relay_b", 3), ("spread", 6),
    ("relay_a", 4), ("second", 0), ("relay_b", 4), ("relay_a", 5), ("spread", 7),
    ("second", 1), ("relay_b", 5), ("hop_b", 3), ("hop_a", 3), ("second", 2),
    ("relay_a", 6), ("hop_a", 4), ("relay_b", 6), ("hop_b", 4), ("relay_z", 0),
    ("relay_a", 7), ("relay_z", 1), ("hop_a", 5), ("hop_b", 5), ("relay_b", 7),
    ("second", 3), ("hop_b", 6), ("hop_a", 6), ("second", 4), ("relay_z", 2),
    ("hop_a", 7), ("hop_b", 7), ("second", 5), ("hop_h", 0), ("second", 6),
    ("relay_z", 3), ("hop_h", 1), ("second", 7), ("finish", 0), ("hop_h", 2),
    ("relay_z", 4), ("relay_z", 5), ("relay_z", 6), ("relay_z", 7), ("hop_h", 4),
    ("hop_h", 3), ("hop_h", 5), ("finish", 6), ("finish", 1), ("finish", 3),
    ("finish", 4), ("finish", 7), ("finish", 2), ("finish", 5),
)
ORDER_FIRST = 0


def local(visibilities, col_offsets, row_offsets, facet_offsets, facet_order, vis_counts):
    vmem, smem = pltpu.VMEM, pltpu.SMEM

    def twice(*shape, chunks=NCH):
        return [vmem((chunks, *shape), BF16), vmem((chunks, *shape), BF16)]

    scratch = [
        vmem((2, M, M), BF16),
        vmem((2, NF, TR, 2 * M), BF16),
        vmem((CH, M), F32), vmem((CH, M), F32),
        vmem((NF, M), F32), vmem((NF, M), F32),
        vmem((CH, M), F32), vmem((CH, M), F32),
        *twice(4, 2, TR, M),
        vmem((NCH, 4, 2, TR, M), F32),
        *twice(2, TR, LA), *twice(2, 2, TR, LA), *twice(TR, LA),
        *twice(4, TR, LB), *twice(TR, LB), *twice(2, TR, LB),
        vmem((NF, M), F32), vmem((NF, M), F32),
        vmem((8, TR, 2 * M), BF16),
        vmem((2 * M, 2 * JB), BF16),
        vmem((NCH, 8, TR, 2 * JB), F32),
        *twice(2, 3, TR, JB), *twice(4, TR, 2 * JB, chunks=len(NOT_MERGED)),
        *twice(9, TR, JB, chunks=len(MERGED)), *twice(TR, JB, chunks=len(NOT_MERGED)),
        vmem((8, 128), F32), vmem((NF - 1, 8, 128), F32),
        pltpu.SemaphoreType.DMA,
        pltpu.SemaphoreType.DMA((len(KINDS) + 1,)), pltpu.SemaphoreType.DMA((NCH, len(KINDS))),
        pltpu.SemaphoreType.DMA, pltpu.SemaphoreType.DMA,
    ]
    images, peak = pl.pallas_call(
        body,
        out_shape=(vmem((1, 2, FR, JB), F32), vmem((8, 128), F32)),
        in_specs=[pl.BlockSpec(memory_space=pl.ANY)] + [pl.BlockSpec(memory_space=smem)] * 5,
        out_specs=(pl.BlockSpec(memory_space=vmem), pl.BlockSpec(memory_space=vmem)),
        scratch_shapes=scratch,
        compiler_params=pltpu.CompilerParams(
            collective_id=0, has_side_effects=True, vmem_limit_bytes=56 * 1024 * 1024
        ),
        name="image_step",
    )(visibilities, col_offsets, row_offsets, facet_offsets.T, facet_order, vis_counts)
    return images, peak[0, :1]


def solution(mesh):
    in_specs = (P(None, "col", "row"), P("col"), P(), P(), P(), P("col", "row"))
    out_specs = (P("col", None, None, "row"), P("col"))
    return jax.shard_map(local, mesh=mesh, in_specs=in_specs, out_specs=out_specs, check_vma=False)
```
